32 devices in a mesh: dp: 4 (over y, x), shard: 8 (over z, core).
Axes of the slice: x: 2, y: 2, z: 4, core: 2. Of those that a mesh axis runs over, the one named last changes fastest.
Arguments:
- gradient: bfloat16 [4, 4096, 6144], P('dp', None, 'shard'), may hold values from -400 to 400
- error_buffer: bfloat16 [4, 4096, 6144], P('dp', None, 'shard'), may hold values from -6 to 6
- right_init: float32 [6144, 32], P('shard'), may hold values from -6 to 6
- first_moment: float32 [4096, 6144], P(('dp', 'shard')), may hold values from -0.06 to 0.06
- second_moment: float32 [4096, 6144], P(('dp', 'shard')), may hold values from 0.001 to 0.01
Outputs:
- error_out: bfloat16 [4, 4096, 6144], P('dp', None, 'shard')
- first_out: float32 [4096, 6144], P(('dp', 'shard'))
- second_out: float32 [4096, 6144], P(('dp', 'shard'))
- direction: float32 [4096, 6144], P(('dp', 'shard'))
The draws below stay inside these ranges and needn't reach their ends.
All inputs are finite; a program needn't handle non-finite values.
Results may differ from the reference program's by a relative error of at most 0.009.
Values sent between devices are 32-bit elements; how exact they have to be, the bound alone decides.
No kernel may reach another device: no remote copies, remote signals or barrier semaphores. Data moves between devices by JAX's collectives and lax.ppermute only.
A program may use at most 64 MiB of HBM per device.

```python
import math
import jax
import jax.numpy as jnp
from jax import lax

D = 4096
F = 6144
R = 32
REPLICAS = 4


def draw_gradient(key, part):
    base = jax.random.fold_in(key, 11)
    key_rows, key_cols, key_sample = jax.random.split(base, 3)
    rising = 6.0 ** (jnp.arange(D, dtype=jnp.float32) / D)
    row_scale = rising * jnp.exp(jax.random.uniform(key_rows, (D,), jnp.float32, 0.0, math.log(10.0) / 4))
    col_scale = jnp.exp(jax.random.uniform(key_cols, (F,), jnp.float32, 0.0, math.log(10.0) / 2))
    sample = jnp.clip(jax.random.normal(key_sample, (REPLICAS, D, F), jnp.float32), -6.0, 6.0)
    factor = jnp.sqrt(jnp.float32(REPLICAS) / 16.0)
    sample = factor * sample
    return (sample * row_scale[None, :, None] * col_scale[None, None, :]).astype(jnp.bfloat16)


def draw_error_buffer(key, part):
    base = jax.random.fold_in(key, 23)
    key_sample = jax.random.fold_in(base, 0)
    factor = jnp.sqrt(jnp.float32(REPLICAS) / 16.0)
    sample = jnp.clip(jax.random.normal(key_sample, (REPLICAS, D, F), jnp.float32), -6.0, 6.0)
    values = factor * sample
    return values.astype(jnp.bfloat16)


def levels(rng, extent, pieces, low, high):
    factor_of = 1.0
    for position, shards_of in pieces:
        heights = jax.random.uniform(jax.random.fold_in(jax.random.fold_in(rng, 6), position), (shards_of,), jnp.float32, low / len(pieces), high / len(pieces))
        factor_of = factor_of * jnp.repeat(jnp.exp(heights), extent[position] // shards_of).reshape((-1,) + (1,) * (len(extent) - 1 - position))
    return factor_of


def normal_values(key, extent, spread, most, cuts=(), held_as=jnp.bfloat16):
    array = jax.random.normal(key, extent, jnp.float32) * spread
    if len(cuts) > 0:
        array = levels(key, extent, cuts, -0.22, 0.18) * array
    return jnp.clip(array, min=-most, max=most).astype(held_as)


def setup_inputs(seed: int = 0) -> dict:
    seeds = jax.random.split(jax.random.key(seed), 6)
    return {
        "gradient": draw_gradient(jax.random.fold_in(seeds[5], 71), 0),
        "error_buffer": draw_error_buffer(jax.random.fold_in(seeds[5], 71), 0),
        "right_init": normal_values(seeds[2], (F, R), 1.0, 6.0, ((0, 8),), jnp.float32),
        "first_moment": normal_values(seeds[3], (D, F), 0.01, 0.06, ((0, 32),), jnp.float32),
        "second_moment": jnp.clip(jnp.exp(math.log(0.01) - 2.30258502 * jax.random.uniform(seeds[4], (D, F), jnp.float32) ** levels(seeds[4], (D, F), ((0, 32),), -0.2, 0.2)), 0.001, 0.01),
    }


CLIP_LEVEL = 0.9
BETA_ONE = 0.9
BETA_TWO = 0.95
EPSILON = 1e-08

def orthonormal(left_raw, gram_matrix):
    width = gram_matrix.shape[0]
    ridge_shift = 1e-06 * jnp.trace(gram_matrix) / width
    lower_factor = jnp.linalg.cholesky(gram_matrix + ridge_shift * jnp.eye(width, dtype=jnp.float32))
    return lax.linalg.triangular_solve(lower_factor, left_raw, left_side=False, lower=True, transpose_a=True)

def merge_pair(items):
    return (items[0].astype(jnp.float32) + items[1].astype(jnp.float32)).astype(jnp.bfloat16)

def reference(gradient, error_buffer, right_init, first_moment, second_moment):
    merged = lax.map(merge_pair, (gradient, error_buffer))
    right_low = right_init.astype(jnp.bfloat16)

    def left_term(matrix):
        return jnp.dot(matrix.astype(jnp.float32), right_low.astype(jnp.float32), preferred_element_type=jnp.float32)
    left_raw = lax.optimization_barrier(jnp.sum(lax.map(left_term, merged), axis=0)) / REPLICAS
    gram_matrix = jnp.dot(left_raw.T, left_raw, precision=lax.Precision.HIGHEST)
    left_orth = orthonormal(left_raw, gram_matrix)
    left_low = left_orth.astype(jnp.bfloat16)

    def right_term(matrix):
        return lax.dot_general(matrix.astype(jnp.float32), left_low.astype(jnp.float32), (((0,), (0,)), ((), ())), preferred_element_type=jnp.float32)
    right_new = lax.optimization_barrier(jnp.sum(lax.map(right_term, merged), axis=0)) / REPLICAS
    update = jnp.dot(left_orth, right_new.T, precision=lax.Precision.HIGHEST)

    def residual(matrix):
        return (matrix.astype(jnp.float32) - update).astype(jnp.bfloat16)
    error_out = lax.map(residual, merged)
    grad_norm = jnp.sqrt(jnp.sum(update * update))
    clip_level = CLIP_LEVEL * jnp.sqrt(jnp.float32(R * (D + F)))
    scaled = update * (clip_level / jnp.maximum(grad_norm, clip_level))
    first_out = BETA_ONE * first_moment + (1.0 - BETA_ONE) * scaled
    second_out = BETA_TWO * second_moment + (1.0 - BETA_TWO) * scaled * scaled
    direction = first_out / (jnp.sqrt(second_out) + EPSILON)
    return (error_out, first_out, second_out, direction)
```

```python
import functools

import jax
import jax.numpy as jnp
from jax import lax
from jax.experimental import pallas as pl
from jax.experimental.pallas import tpu as pltpu
from jax.sharding import PartitionSpec as P

CLIP_LEVEL = 0.9
BETA_ONE = 0.9
BETA_TWO = 0.95
EPSILON = 1e-08
CORES = 2
MIB = 1 << 20


f32, bf16 = jnp.float32, jnp.bfloat16
HIGHEST = lax.Precision.HIGHEST
VMEM = pl.BlockSpec(memory_space=pltpu.VMEM)


def to_peer(i, k, n):
    return i ^ k if n & (n - 1) == 0 else lax.rem(i + k, n) if isinstance(i, jax.Array) else (i + k) % n


def from_peer(i, k, n):
    return i ^ k if n & (n - 1) == 0 else lax.rem(i + n - k, n) if isinstance(i, jax.Array) else (i + n - k) % n


def params(mib, grid=False):
    extra = {"dimension_semantics": ("arbitrary",)} if grid else {}
    return pltpu.CompilerParams(vmem_limit_bytes=mib * MIB, **extra)


def cost(flops, moved):
    return pl.CostEstimate(flops=flops, bytes_accessed=moved, transcendentals=0)


def split2(x):
    high = x.astype(bf16)
    return high, (x - high.astype(f32)).astype(bf16)


def split3(x):
    high = x.astype(bf16)
    rest = x - high.astype(f32)
    mid = rest.astype(bf16)
    return high, mid, (rest - mid.astype(f32)).astype(bf16)


def lanes(start, size, align):
    return pl.ds(pl.multiple_of(start, align) if align else start, size)


def merge_kernel(half_blocks, g_ref, e_ref, q_ref, merged_ref, mine_ref, other_ref):
    i = pl.program_id(0)
    rows = g_ref.shape[0]
    core = lax.rem(lax.axis_index("shard"), CORES)
    merged = (g_ref[...].astype(f32) + e_ref[...].astype(f32)).astype(bf16)
    merged_ref[pl.ds(pl.multiple_of(i * rows, rows), rows), :] = merged
    left = lax.dot_general(
        q_ref[...].astype(bf16), merged, (((1,), (1,)), ((), ())), preferred_element_type=f32
    )
    owner = i // half_blocks
    place = pl.ds(pl.multiple_of(lax.rem(i, half_blocks) * rows, rows), rows)

    @pl.when(owner == core)
    def _():
        mine_ref[:, place] = left

    @pl.when(owner != core)
    def _():
        other_ref[:, place] = left


def cut_kernel(n_dp, mine_ref, got_ref, *out_refs):
    me = lax.axis_index("dp")
    width = out_refs[0].shape[1]
    for k in range(n_dp):
        place = lanes(to_peer(me, k, n_dp) * width, width, width)
        out_refs[k][...] = mine_ref[:, place] + got_ref[:, place]


def piece_rows(n_dp, width, k, partner):
    me = lax.axis_index("dp")
    core = lax.rem(lax.axis_index("shard"), CORES)
    owner = (1 - core) if partner else core
    return pl.multiple_of((owner * n_dp + from_peer(me, k, n_dp)) * width, width)


def right_kernel(n_dp, *refs):
    merged_ref, out_ref = refs[2 * n_dp], refs[2 * n_dp + 1]
    width = refs[0].shape[1]
    rank = refs[0].shape[0]
    total = jnp.zeros((3 * rank, out_ref.shape[1]), f32)
    for index in range(2 * n_dp):
        rows = piece_rows(n_dp, width, index % n_dp, index >= n_dp)
        terms = jnp.concatenate(split3(refs[index][...]), axis=0)
        total += jnp.dot(terms, merged_ref[pl.ds(rows, width), :], preferred_element_type=f32)
    out_ref[...] = total[:rank] + total[rank : 2 * rank] + total[2 * rank :]


def factor_kernel(n_dp, *refs):
    inverse_ref, gram_ref, high_ref, low_ref = refs[2 * n_dp :]
    width = refs[0].shape[1]
    rank = refs[0].shape[0]
    total = jnp.zeros((3 * rank, 3 * rank), f32)
    for index in range(2 * n_dp):
        terms = jnp.concatenate(split3(refs[index][...]), axis=0)
        total += lax.dot_general(terms, terms, (((1,), (1,)), ((), ())), preferred_element_type=f32)
    gram = jnp.zeros((rank, rank), f32)
    for a in range(3):
        for b in range(3):
            gram += total[a * rank : (a + 1) * rank, b * rank : (b + 1) * rank]
    row_id = lax.broadcasted_iota(jnp.int32, (rank, rank), 0)
    col_id = lax.broadcasted_iota(jnp.int32, (rank, rank), 1)
    unit = (row_id == col_id).astype(f32)
    ridge = 1e-06 * jnp.sum(gram * unit) / rank
    both = jnp.concatenate([gram + ridge * unit, unit], axis=1)
    below = lax.broadcasted_iota(jnp.int32, (rank, 1), 0)
    for j in range(rank - 1):
        factor = both[:, j : j + 1] / both[j : j + 1, j : j + 1]
        both = both - jnp.where(below > j, factor, 0.0) * both[j : j + 1, :]
    pivots = jnp.sum(both[:, :rank] * unit, axis=1, keepdims=True)
    inverse = both[:, rank:] / jnp.sqrt(pivots)
    inverse_ref[...] = inverse
    total = jnp.zeros((2 * rank, 2 * rank), f32)
    for index in range(2 * n_dp):
        rows = piece_rows(n_dp, width, index % n_dp, index >= n_dp)
        orth = jnp.dot(inverse, refs[index][...], precision=HIGHEST, preferred_element_type=f32)
        high, low = split2(orth)
        high_ref[:, pl.ds(rows, width)] = high
        low_ref[:, pl.ds(rows, width)] = low
        terms = jnp.concatenate([high, low], axis=0)
        total += lax.dot_general(terms, terms, (((1,), (1,)), ((), ())), preferred_element_type=f32)
    gram_ref[...] = (
        total[:rank, :rank] + total[:rank, rank:] + total[rank:, :rank] + total[rank:, rank:]
    )


def solve_kernel(n_dp, inverse_ref, *refs):
    out_ref = refs[n_dp]
    total = refs[0][...]
    for k in range(1, n_dp):
        total += refs[k][...]
    out_ref[...] = jnp.dot(
        inverse_ref[...], total / n_dp, precision=HIGHEST, preferred_element_type=f32
    )


def stacked_left(high, low):
    return jnp.concatenate([high, high, low], axis=0)


def stacked_right(right):
    high, low = split2(right)
    return jnp.concatenate([high, low, high], axis=0)


def product(left3, right3):
    return lax.dot_general(left3, right3, (((0,), (0,)), ((), ())), preferred_element_type=f32)


def residual_kernel(high_ref, low_ref, right_ref, merged_ref, out_ref, right3_ref):
    i = pl.program_id(0)
    rows = out_ref.shape[1]

    @pl.when(i == 0)
    def _():
        right3_ref[...] = stacked_right(right_ref[...])

    place = pl.ds(pl.multiple_of(i * rows, rows), rows)
    update = product(stacked_left(high_ref[:, place], low_ref[:, place]), right3_ref[...])
    out_ref[0] = (merged_ref[place, :].astype(f32) - update).astype(bf16)


def adam_kernel(n_blocks, clip_level, high_ref, low_ref, gram_ref, *refs):
    right_refs = refs[:n_blocks]
    first_ref, second_ref, first_out, second_out, direction_out, right3_ref, ratio_ref = refs[n_blocks:]
    i = pl.program_id(0)
    rank = gram_ref.shape[0]

    @pl.when(i == 0)
    def _():
        total = jnp.zeros((2 * rank, 2 * rank), f32)
        for k in range(n_blocks):
            stacked = stacked_right(right_refs[k][...])
            right3_ref[k] = stacked
            terms = stacked[: 2 * rank]
            total += lax.dot_general(
                terms, terms, (((1,), (1,)), ((), ())), preferred_element_type=f32
            )
        right_gram = (
            total[:rank, :rank] + total[:rank, rank:] + total[rank:, :rank] + total[rank:, rank:]
        )
        norm = jnp.sqrt(jnp.full((1, 128), jnp.sum(right_gram * gram_ref[...]), f32))
        ratio_ref[...] = clip_level / jnp.maximum(norm, clip_level)

    update = product(stacked_left(high_ref[...], low_ref[...]), right3_ref[i])
    scaled = update * ratio_ref[0:1, 0:1]
    first = BETA_ONE * first_ref[...] + (1.0 - BETA_ONE) * scaled
    second = BETA_TWO * second_ref[...] + (1.0 - BETA_TWO) * scaled * scaled
    first_out[...] = first
    second_out[...] = second
    direction_out[...] = first / (jnp.sqrt(second) + EPSILON)


def local(gradient, error_buffer, right_init, first_moment, second_moment):
    n_dp = lax.axis_size("dp")
    n_shard = lax.axis_size("shard")
    n_z = n_shard // CORES
    depth, cols = gradient.shape[1:]
    rank = right_init.shape[1]
    half = depth // CORES
    width = half // n_dp
    own = first_moment.shape[0]
    total_cols = first_moment.shape[1]

    def swap_cores(x):
        return lax.ppermute(x, "shard", [(i, i ^ 1) for i in range(n_shard)])

    def send_dp(x, k):
        return lax.ppermute(x, "dp", [(i, to_peer(i, k, n_dp)) for i in range(n_dp)])

    def send_z(x, k):
        pairs = [(i, to_peer(i // CORES, k, n_z) * CORES + i % CORES) for i in range(n_shard)]
        return lax.ppermute(x, "shard", pairs)

    rows = min(512, half)
    block = pl.BlockSpec((None, rows, cols), lambda i: (0, i, 0))
    merged, mine, other = pl.pallas_call(
        functools.partial(merge_kernel, half // rows),
        grid=(depth // rows,),
        in_specs=[block, block, VMEM],
        out_specs=[VMEM, VMEM, VMEM],
        out_shape=[
            pltpu.VMEM((depth, cols), bf16),
            pltpu.VMEM((rank, half), f32),
            pltpu.VMEM((rank, half), f32),
        ],
        compiler_params=params(16, True),
        cost_estimate=cost(4 * depth * cols * rank, 6 * depth * cols),
        name="merge",
    )(gradient, error_buffer, right_init.T)

    got = swap_cores(other)
    pieces = pl.pallas_call(
        functools.partial(cut_kernel, n_dp),
        in_specs=[VMEM, VMEM],
        out_specs=[VMEM] * n_dp,
        out_shape=[pltpu.VMEM((rank, width), f32)] * n_dp,
        compiler_params=params(4),
        name="cut",
    )(mine, got)
    partial = pieces[0]
    for arrived in [send_dp(pieces[k], k) for k in range(1, n_dp)]:
        partial = partial + arrived
    total = partial
    for arrived in [send_z(partial, k) for k in range(1, n_z)]:
        total = total + arrived
    total = total / n_dp
    lefts = [total] + [send_dp(total, k) for k in range(1, n_dp)]
    lefts = lefts + [swap_cores(x) for x in lefts]

    right_part = pl.pallas_call(
        functools.partial(right_kernel, n_dp),
        in_specs=[VMEM] * (2 * n_dp + 1),
        out_specs=VMEM,
        out_shape=pltpu.VMEM((rank, cols), f32),
        compiler_params=params(8),
        cost_estimate=cost(6 * depth * cols * rank, depth * cols),
        name="right",
    )(*lefts, merged)
    right_parts = [right_part] + [send_dp(right_part, k) for k in range(1, n_dp)]
    inverse, gram, high, low = pl.pallas_call(
        functools.partial(factor_kernel, n_dp),
        in_specs=[VMEM] * (2 * n_dp),
        out_specs=[VMEM] * 4,
        out_shape=[
            pltpu.VMEM((rank, rank), f32),
            pltpu.VMEM((rank, rank), f32),
            pltpu.VMEM((rank, depth), bf16),
            pltpu.VMEM((rank, depth), bf16),
        ],
        compiler_params=params(8),
        cost_estimate=cost(200 * depth * rank * rank, depth * rank * 8),
        name="factor",
    )(*lefts)
    right = pl.pallas_call(
        functools.partial(solve_kernel, n_dp),
        in_specs=[VMEM] * (n_dp + 1),
        out_specs=VMEM,
        out_shape=pltpu.VMEM((rank, cols), f32),
        compiler_params=params(4),
        name="solve",
    )(inverse, *right_parts)

    rights = [right] + [send_z(right, k) for k in range(1, n_z)]
    rights = rights + [swap_cores(x) for x in rights]

    error_out = pl.pallas_call(
        residual_kernel,
        grid=(depth // rows,),
        in_specs=[VMEM] * 4,
        out_specs=pl.BlockSpec((1, rows, cols), lambda i: (0, i, 0)),
        out_shape=jax.ShapeDtypeStruct((1, depth, cols), bf16),
        scratch_shapes=[pltpu.VMEM((3 * rank, cols), bf16)],
        compiler_params=params(12, True),
        cost_estimate=cost(16 * depth * cols * rank, 4 * depth * cols),
        name="residual",
    )(high, low, right, merged)

    first_row = (lax.axis_index("dp") * n_shard + lax.axis_index("shard")) * own
    own_high = lax.dynamic_slice_in_dim(high, first_row, own, 1)
    own_low = lax.dynamic_slice_in_dim(low, first_row, own, 1)

    def column_block(i):
        shard = lax.axis_index("shard")
        core, z = lax.rem(shard, CORES), shard // CORES
        owner = jnp.where(i >= n_z, 1 - core, core)
        return (0, from_peer(z, lax.rem(i, n_z), n_z) * CORES + owner)

    moment = pl.BlockSpec((own, cols), column_block)
    clip_level = CLIP_LEVEL * float(rank * (depth + total_cols)) ** 0.5
    first_out, second_out, direction = pl.pallas_call(
        functools.partial(adam_kernel, n_shard, clip_level),
        grid=(n_shard,),
        in_specs=[VMEM] * (3 + n_shard) + [moment, moment],
        out_specs=[moment] * 3,
        out_shape=[jax.ShapeDtypeStruct(first_moment.shape, f32)] * 3,
        scratch_shapes=[
            pltpu.VMEM((n_shard, 3 * rank, cols), bf16),
            pltpu.VMEM((1, 128), f32),
        ],
        compiler_params=params(12, True),
        cost_estimate=cost(16 * own * total_cols * rank, 20 * own * total_cols),
        name="adam",
    )(own_high, own_low, gram, *rights, first_moment, second_moment)
    return (error_out, first_out, second_out, direction)


def solution(mesh):
    return jax.shard_map(
        local,
        mesh=mesh,
        in_specs=(
            P("dp", None, "shard"),
            P("dp", None, "shard"),
            P("shard", None),
            P(("dp", "shard"), None),
            P(("dp", "shard"), None),
        ),
        out_specs=(
            P("dp", None, "shard"),
            P(("dp", "shard"), None),
            P(("dp", "shard"), None),
            P(("dp", "shard"), None),
        ),
        check_vma=False,
    )
```

```python
import functools

import jax
import jax.numpy as jnp
from jax import lax
from jax.experimental import pallas as pl
from jax.experimental.pallas import tpu as pltpu
from jax.sharding import PartitionSpec as P

CLIP_LEVEL = 0.9
BETA_ONE = 0.9
BETA_TWO = 0.95
EPSILON = 1e-08
CORES = 2
ADAM_ROWS = 64
MIB = 1 << 20


f32, bf16 = jnp.float32, jnp.bfloat16
HIGHEST = lax.Precision.HIGHEST
VMEM = pl.BlockSpec(memory_space=pltpu.VMEM)
ANY = pl.BlockSpec(memory_space=pl.ANY)


def to_peer(i, k, n):
    return i ^ k if n & (n - 1) == 0 else lax.rem(i + k, n) if isinstance(i, jax.Array) else (i + k) % n


def from_peer(i, k, n):
    return i ^ k if n & (n - 1) == 0 else lax.rem(i + n - k, n) if isinstance(i, jax.Array) else (i + n - k) % n


def params(mib, grid=False):
    extra = {"dimension_semantics": ("arbitrary",)} if grid else {}
    return pltpu.CompilerParams(vmem_limit_bytes=mib * MIB, **extra)


def cost(flops, moved):
    return pl.CostEstimate(flops=flops, bytes_accessed=moved, transcendentals=0)


def split2(x):
    high = x.astype(bf16)
    return high, (x - high.astype(f32)).astype(bf16)


def split3(x):
    high = x.astype(bf16)
    rest = x - high.astype(f32)
    mid = rest.astype(bf16)
    return high, mid, (rest - mid.astype(f32)).astype(bf16)


def in_hbm(x):
    return pltpu.with_memory_space_constraint(x, pltpu.HBM)


def in_vmem(x):
    return pltpu.with_memory_space_constraint(x, pltpu.VMEM)


def lanes(start, size, align):
    return pl.ds(pl.multiple_of(start, align) if align else start, size)


def merge_kernel(chunks, g_ref, e_ref, q_ref, merged_ref, mine_ref, other_ref, error_ref, right_ref, sems):
    rows = merged_ref.shape[0] // chunks
    right_copy = pltpu.make_async_copy(q_ref, right_ref, sems.at[2, 0])
    right_copy.start()
    copies = []
    for i in range(chunks):
        place = pl.ds(i * rows, rows)
        pair = (
            pltpu.make_async_copy(g_ref.at[0, place, :], merged_ref.at[place, :], sems.at[0, i]),
            pltpu.make_async_copy(e_ref.at[0, place, :], error_ref.at[place, :], sems.at[1, i]),
        )
        for copy in pair:
            copy.start()
        copies.append(pair)
    core = lax.rem(lax.axis_index("shard"), CORES)
    right_copy.wait()
    right = right_ref[...].astype(bf16)
    half = chunks // CORES
    for i in range(chunks):
        for copy in copies[i]:
            copy.wait()
        place = pl.ds(i * rows, rows)
        merged = (merged_ref[place, :].astype(f32) + error_ref[place, :].astype(f32)).astype(bf16)
        merged_ref[place, :] = merged
        left = lax.dot_general(right, merged, (((1,), (1,)), ((), ())), preferred_element_type=f32)
        owner, place = i // half, pl.ds((i % half) * rows, rows)

        @pl.when(core == owner)
        def _():
            mine_ref[:, place] = left

        @pl.when(core != owner)
        def _():
            other_ref[:, place] = left


def cut_kernel(n_dp, mine_ref, got_ref, *out_refs):
    me = lax.axis_index("dp")
    width = out_refs[0].shape[1]
    for k in range(n_dp):
        place = lanes(to_peer(me, k, n_dp) * width, width, width)
        out_refs[k][...] = mine_ref[:, place] + got_ref[:, place]


def piece_rows(n_dp, width, k, partner):
    me = lax.axis_index("dp")
    core = lax.rem(lax.axis_index("shard"), CORES)
    owner = (1 - core) if partner else core
    return pl.multiple_of((owner * n_dp + from_peer(me, k, n_dp)) * width, width)


def right_kernel(n_dp, *refs):
    merged_ref, out_ref = refs[2 * n_dp], refs[2 * n_dp + 1]
    width = refs[0].shape[1]
    rank = refs[0].shape[0]
    total = jnp.zeros((3 * rank, out_ref.shape[1]), f32)
    for index in range(2 * n_dp):
        rows = piece_rows(n_dp, width, index % n_dp, index >= n_dp)
        terms = jnp.concatenate(split3(refs[index][...]), axis=0)
        total += jnp.dot(terms, merged_ref[pl.ds(rows, width), :], preferred_element_type=f32)
    out_ref[...] = total[:rank] + total[rank : 2 * rank] + total[2 * rank :]


def factor_kernel(n_dp, *refs):
    inverse_ref, gram_ref, high_ref, low_ref = refs[2 * n_dp :]
    width = refs[0].shape[1]
    rank = refs[0].shape[0]
    total = jnp.zeros((3 * rank, 3 * rank), f32)
    for index in range(2 * n_dp):
        terms = jnp.concatenate(split3(refs[index][...]), axis=0)
        total += lax.dot_general(terms, terms, (((1,), (1,)), ((), ())), preferred_element_type=f32)
    gram = jnp.zeros((rank, rank), f32)
    for a in range(3):
        for b in range(3):
            gram += total[a * rank : (a + 1) * rank, b * rank : (b + 1) * rank]
    row_id = lax.broadcasted_iota(jnp.int32, (rank, rank), 0)
    col_id = lax.broadcasted_iota(jnp.int32, (rank, rank), 1)
    unit = (row_id == col_id).astype(f32)
    ridge = 1e-06 * jnp.sum(gram * unit) / rank
    both = jnp.concatenate([gram + ridge * unit, unit], axis=1)
    below = lax.broadcasted_iota(jnp.int32, (rank, 1), 0)
    for j in range(rank - 1):
        factor = both[:, j : j + 1] / both[j : j + 1, j : j + 1]
        both = both - jnp.where(below > j, factor, 0.0) * both[j : j + 1, :]
    pivots = jnp.sum(both[:, :rank] * unit, axis=1, keepdims=True)
    inverse = both[:, rank:] / jnp.sqrt(pivots)
    inverse_ref[...] = inverse
    gram_ref[...] = unit - ridge * lax.dot_general(
        inverse, inverse, (((1,), (1,)), ((), ())), precision=HIGHEST, preferred_element_type=f32
    )
    inverse2 = jnp.concatenate(split2(inverse), axis=0)
    for index in range(2 * n_dp):
        rows = piece_rows(n_dp, width, index % n_dp, index >= n_dp)
        high, low = split2(refs[index][...])
        first = jnp.dot(inverse2, high, preferred_element_type=f32)
        second = jnp.dot(inverse2[:rank], low, preferred_element_type=f32)
        high, low = split2(first[:rank] + (first[rank:] + second))
        high_ref[:, pl.ds(rows, width)] = high
        low_ref[:, pl.ds(rows, width)] = low


def solve_kernel(n_dp, inverse_ref, *refs):
    out_ref = refs[n_dp + 2]
    total = refs[0][...]
    for k in range(1, n_dp):
        total += refs[k][...]
    out_ref[...] = jnp.dot(
        inverse_ref[...], total / n_dp, precision=HIGHEST, preferred_element_type=f32
    )


def stacked_left(high, low):
    return jnp.concatenate([high, high, low], axis=0)


def stacked_right(right):
    high, low = split2(right)
    return jnp.concatenate([high, low, high], axis=0)


def product(left3, right3):
    return lax.dot_general(left3, right3, (((0,), (0,)), ((), ())), preferred_element_type=f32)


def residual_kernel(chunks, high_ref, low_ref, right_ref, merged_ref, out_ref, error_ref, sems):
    rows = error_ref.shape[0] // chunks
    right3 = stacked_right(right_ref[...])
    copies = []
    for i in range(chunks):
        place = pl.ds(i * rows, rows)
        update = product(stacked_left(high_ref[:, place], low_ref[:, place]), right3)
        error_ref[place, :] = (merged_ref[place, :].astype(f32) - update).astype(bf16)
        copy = pltpu.make_async_copy(error_ref.at[place, :], out_ref.at[0, place, :], sems.at[i])
        copy.start()
        copies.append(copy)
    for copy in copies:
        copy.wait()


def own_left(own, high_ref, low_ref):
    if own % 128:
        return stacked_left(high_ref[...], low_ref[...])
    place = lax.axis_index("dp") * lax.axis_size("shard") + lax.axis_index("shard")
    place = lanes(place * own, own, own)
    return stacked_left(high_ref[:, place], low_ref[:, place])


def rows_kernel(high_ref, low_ref, *refs):
    *right_refs, update_ref, gram_ref = refs
    rank, cols = right_refs[0].shape
    left = own_left(update_ref.shape[0], high_ref, low_ref)
    total = jnp.zeros((2 * rank, 2 * rank), f32)
    for k, ref in enumerate(right_refs):
        right = stacked_right(ref[...])
        terms = right[: 2 * rank]
        total += lax.dot_general(terms, terms, (((1,), (1,)), ((), ())), preferred_element_type=f32)
        update_ref[:, k * cols : (k + 1) * cols] = product(left, right)
    gram_ref[...] = total[:rank, :rank] + total[:rank, rank:] + total[rank:, :rank] + total[rank:, rank:]


def adam_kernel(n_z, clip_level, high_ref, low_ref, gram_ref, here_ref, here_gram_ref, *refs):
    right_refs = refs[:n_z]
    first_ref, second_ref, *outs = refs[n_z : n_z + 5]
    *bufs, there_ref, there_gram_ref, sems = refs[n_z + 5 :]
    cols = right_refs[0].shape[1]
    own = first_ref.shape[0]
    shard = lax.axis_index("shard")
    core, z = lax.rem(shard, CORES), shard // CORES
    rows_kernel(high_ref, low_ref, *right_refs, there_ref, there_gram_ref)
    square = (here_gram_ref[...] + there_gram_ref[...]) * gram_ref[...]
    square = jnp.sum(jnp.sum(square, axis=0, keepdims=True), axis=1, keepdims=True)
    ratio = clip_level / jnp.maximum(jnp.sqrt(square), clip_level)
    first_factor = (1.0 - BETA_ONE) * ratio
    second_factor = (1.0 - BETA_TWO) * ratio * ratio
    step = min(ADAM_ROWS, own)

    def copies(k, partner):
        owner = 1 - core if partner else core
        column = pl.multiple_of((from_peer(z, k, n_z) * CORES + owner) * cols, cols)
        place = pl.ds(column, cols)
        return place, [
            pltpu.make_async_copy(
                bufs[j].at[:, place], outs[j].at[:, place], sems.at[j, k + n_z * partner]
            )
            for j in range(3)
        ]

    for partner, update_ref in ((0, here_ref), (1, there_ref)):

        def block(k, carry):
            place, block_copies = copies(k, partner)
            source = pl.ds(pl.multiple_of(k * cols, cols), cols)

            def tile(t, carry):
                rows = pl.ds(pl.multiple_of(t * step, step), step)
                update = update_ref[rows, source]
                first = BETA_ONE * first_ref[rows, place] + first_factor * update
                second = BETA_TWO * second_ref[rows, place] + second_factor * (update * update)
                bufs[0][rows, place] = first
                bufs[1][rows, place] = second
                bufs[2][rows, place] = first / (second * lax.rsqrt(second) + EPSILON)
                return carry

            lax.fori_loop(0, own // step, tile, 0)
            for copy in block_copies:
                copy.start()
            return carry

        lax.fori_loop(0, n_z, block, 0)
    for partner in range(CORES):
        for k in range(n_z):
            for copy in copies(k, partner)[1]:
                copy.wait()


def local(gradient, error_buffer, right_init, first_moment, second_moment):
    n_dp = lax.axis_size("dp")
    n_shard = lax.axis_size("shard")
    n_z = n_shard // CORES
    depth, cols = gradient.shape[1:]
    rank = right_init.shape[1]
    half = depth // CORES
    width = half // n_dp
    own = first_moment.shape[0]
    total_cols = first_moment.shape[1]

    def swap_cores(x):
        return lax.ppermute(x, "shard", [(i, i ^ 1) for i in range(n_shard)])

    def send_dp(x, k):
        return lax.ppermute(x, "dp", [(i, to_peer(i, k, n_dp)) for i in range(n_dp)])

    def send_z(x, k):
        pairs = [(i, to_peer(i // CORES, k, n_z) * CORES + i % CORES) for i in range(n_shard)]
        return lax.ppermute(x, "shard", pairs)

    chunks = 8
    merged, mine, other = pl.pallas_call(
        functools.partial(merge_kernel, chunks),
        in_specs=[ANY] * 3,
        out_specs=[VMEM] * 3,
        out_shape=[
            pltpu.VMEM((depth, cols), bf16),
            pltpu.VMEM((rank, half), f32),
            pltpu.VMEM((rank, half), f32),
        ],
        scratch_shapes=[
            pltpu.VMEM((depth, cols), bf16),
            pltpu.VMEM((rank, cols), f32),
            pltpu.SemaphoreType.DMA((3, chunks)),
        ],
        compiler_params=params(12),
        cost_estimate=cost(4 * depth * cols * rank, 6 * depth * cols),
        name="merge",
    )(in_hbm(gradient), in_hbm(error_buffer), in_hbm(right_init.T))

    got = swap_cores(other)
    pieces = pl.pallas_call(
        functools.partial(cut_kernel, n_dp),
        in_specs=[VMEM, VMEM],
        out_specs=[VMEM] * n_dp,
        out_shape=[pltpu.VMEM((rank, width), f32)] * n_dp,
        compiler_params=params(4),
        name="cut",
    )(mine, got)
    partial = pieces[0]
    for arrived in [send_dp(pieces[k], k) for k in range(1, n_dp)]:
        partial = partial + arrived
    total = partial
    for arrived in [send_z(partial, k) for k in range(1, n_z)]:
        total = total + arrived
    total = total / n_dp
    lefts = [total] + [send_dp(total, k) for k in range(1, n_dp)]
    lefts = lefts + [swap_cores(x) for x in lefts]

    right_part = pl.pallas_call(
        functools.partial(right_kernel, n_dp),
        in_specs=[VMEM] * (2 * n_dp + 1),
        out_specs=VMEM,
        out_shape=pltpu.VMEM((rank, cols), f32),
        compiler_params=params(8),
        cost_estimate=cost(6 * depth * cols * rank, depth * cols),
        name="right",
    )(*lefts, merged)
    right_parts = [right_part] + [send_dp(right_part, k) for k in range(1, n_dp)]
    inverse, gram, high, low = pl.pallas_call(
        functools.partial(factor_kernel, n_dp),
        in_specs=[VMEM] * (2 * n_dp),
        out_specs=[VMEM] * 4,
        out_shape=[
            pltpu.VMEM((rank, rank), f32),
            pltpu.VMEM((rank, rank), f32),
            pltpu.VMEM((rank, depth), bf16),
            pltpu.VMEM((rank, depth), bf16),
        ],
        compiler_params=params(8),
        cost_estimate=cost(200 * depth * rank * rank, depth * rank * 8),
        name="factor",
    )(*lefts)
    first_here, second_here = in_vmem(first_moment), in_vmem(second_moment)
    right = pl.pallas_call(
        functools.partial(solve_kernel, n_dp),
        in_specs=[VMEM] * (n_dp + 3),
        out_specs=VMEM,
        out_shape=pltpu.VMEM((rank, cols), f32),
        compiler_params=params(16),
        name="solve",
    )(inverse, *right_parts, first_here, second_here)

    swapped = [swap_cores(right)]
    rights = [right] + [send_z(right, k) for k in range(1, n_z)]
    residual_chunks = 8
    error_out = pl.pallas_call(
        functools.partial(residual_kernel, residual_chunks),
        in_specs=[VMEM] * 4,
        out_specs=ANY,
        out_shape=pltpu.HBM((1, depth, cols), bf16),
        scratch_shapes=[pltpu.VMEM((depth, cols), bf16), pltpu.SemaphoreType.DMA((residual_chunks,))],
        compiler_params=params(12),
        cost_estimate=cost(16 * depth * cols * rank, 4 * depth * cols),
        name="residual",
    )(high, low, right, in_vmem(merged))
    *arrived, error_out = lax.optimization_barrier((*rights[1:], error_out))
    rights = [right] + arrived
    swapped = swapped + [swap_cores(x) for x in arrived]

    if own % 128:
        first_row = (lax.axis_index("dp") * n_shard + lax.axis_index("shard")) * own
        high = lax.dynamic_slice_in_dim(high, first_row, own, 1)
        low = lax.dynamic_slice_in_dim(low, first_row, own, 1)
    clip_level = CLIP_LEVEL * float(rank * (depth + total_cols)) ** 0.5
    here, here_gram = pl.pallas_call(
        rows_kernel,
        in_specs=[VMEM] * (2 + n_z),
        out_specs=[VMEM] * 2,
        out_shape=[pltpu.VMEM((own, n_z * cols), f32), pltpu.VMEM((rank, rank), f32)],
        compiler_params=params(8),
        cost_estimate=cost(16 * own * total_cols * rank, 4 * own * total_cols),
        name="rows",
    )(high, low, *rights)
    first_out, second_out, direction = pl.pallas_call(
        functools.partial(adam_kernel, n_z, clip_level),
        in_specs=[VMEM] * (7 + n_z),
        out_specs=[ANY] * 3,
        out_shape=[pltpu.HBM(first_moment.shape, f32)] * 3,
        scratch_shapes=[pltpu.VMEM(first_moment.shape, f32)] * 3
        + [
            pltpu.VMEM((own, n_z * cols), f32),
            pltpu.VMEM((rank, rank), f32),
            pltpu.SemaphoreType.DMA((3, n_shard)),
        ],
        compiler_params=params(24),
        cost_estimate=cost(16 * own * total_cols * rank, 20 * own * total_cols),
        name="adam",
    )(high, low, gram, here, here_gram, *swapped, first_here, second_here)
    return (error_out, first_out, second_out, direction)


def solution(mesh):
    return jax.shard_map(
        local,
        mesh=mesh,
        in_specs=(
            P("dp", None, "shard"),
            P("dp", None, "shard"),
            P("shard", None),
            P(("dp", "shard"), None),
            P(("dp", "shard"), None),
        ),
        out_specs=(
            P("dp", None, "shard"),
            P(("dp", "shard"), None),
            P(("dp", "shard"), None),
            P(("dp", "shard"), None),
        ),
        check_vma=False,
    )
```

```python
import functools

import jax
import jax.numpy as jnp
from jax import lax
from jax.experimental import pallas as pl
from jax.experimental.pallas import tpu as pltpu
from jax.sharding import PartitionSpec as P


CLIP_LEVEL = 0.9
BETA_ONE = 0.9
BETA_TWO = 0.95
EPSILON = 1e-08
CORES = 2
ADAM_ROWS = 32
MIB = 1 << 20


f32, bf16 = jnp.float32, jnp.bfloat16
HIGHEST = lax.Precision.HIGHEST
VMEM = pl.BlockSpec(memory_space=pltpu.VMEM)
ANY = pl.BlockSpec(memory_space=pl.ANY)


def to_peer(i, k, n):
    return i ^ k if n & (n - 1) == 0 else lax.rem(i + k, n) if isinstance(i, jax.Array) else (i + k) % n


def from_peer(i, k, n):
    return i ^ k if n & (n - 1) == 0 else lax.rem(i + n - k, n) if isinstance(i, jax.Array) else (i + n - k) % n


def params(mib, grid=False):
    extra = {"dimension_semantics": ("arbitrary",)} if grid else {}
    return pltpu.CompilerParams(vmem_limit_bytes=mib * MIB, **extra)


def cost(flops, moved):
    return pl.CostEstimate(flops=flops, bytes_accessed=moved, transcendentals=0)


def split2(x):
    high = x.astype(bf16)
    return high, (x - high.astype(f32)).astype(bf16)


def split3(x):
    high = x.astype(bf16)
    rest = x - high.astype(f32)
    mid = rest.astype(bf16)
    return high, mid, (rest - mid.astype(f32)).astype(bf16)


def in_hbm(x):
    return pltpu.with_memory_space_constraint(x, pltpu.HBM)


def in_vmem(x):
    return pltpu.with_memory_space_constraint(x, pltpu.VMEM)


def lanes(start, size, align):
    return pl.ds(pl.multiple_of(start, align) if align else start, size)


def merge_kernel(chunks, g_ref, e_ref, q_ref, merged_ref, mine_ref, other_ref, error_ref, right_ref, sems):
    rows = merged_ref.shape[0] // chunks
    right_copy = pltpu.make_async_copy(q_ref, right_ref, sems.at[2, 0])
    right_copy.start()
    copies = []
    for i in range(chunks):
        place = pl.ds(i * rows, rows)
        pair = (
            pltpu.make_async_copy(g_ref.at[0, place, :], merged_ref.at[place, :], sems.at[0, i]),
            pltpu.make_async_copy(e_ref.at[0, place, :], error_ref.at[place, :], sems.at[1, i]),
        )
        for copy in pair:
            copy.start()
        copies.append(pair)
    core = lax.rem(lax.axis_index("shard"), CORES)
    right_copy.wait()
    right = right_ref[...].astype(bf16)
    half = chunks // CORES
    for i in range(chunks):
        for copy in copies[i]:
            copy.wait()
        place = pl.ds(i * rows, rows)
        merged = (merged_ref[place, :].astype(f32) + error_ref[place, :].astype(f32)).astype(bf16)
        merged_ref[place, :] = merged
        left = lax.dot_general(right, merged, (((1,), (1,)), ((), ())), preferred_element_type=f32)
        owner, place = i // half, pl.ds((i % half) * rows, rows)

        @pl.when(core == owner)
        def _():
            mine_ref[:, place] = left

        @pl.when(core != owner)
        def _():
            other_ref[:, place] = left


def cut_kernel(n_dp, mine_ref, got_ref, *out_refs):
    me = lax.axis_index("dp")
    width = out_refs[0].shape[1]
    for k in range(n_dp):
        place = lanes(to_peer(me, k, n_dp) * width, width, width)
        out_refs[k][...] = mine_ref[:, place] + got_ref[:, place]


def piece_rows(n_dp, width, k, partner):
    me = lax.axis_index("dp")
    core = lax.rem(lax.axis_index("shard"), CORES)
    owner = (1 - core) if partner else core
    return pl.multiple_of((owner * n_dp + from_peer(me, k, n_dp)) * width, width)


def right_kernel(n_dp, partner, *refs):
    merged_ref, *sum_ref, out_ref = refs[n_dp:]
    rank, width = refs[0].shape
    total = jnp.zeros((3 * rank, out_ref.shape[1]), f32)
    for k in range(n_dp):
        rows = piece_rows(n_dp, width, k, partner)
        terms = jnp.concatenate(split3(refs[k][...]), axis=0)
        total += jnp.dot(terms, merged_ref[pl.ds(rows, width), :], preferred_element_type=f32)
    total = total[:rank] + total[rank : 2 * rank] + total[2 * rank :]
    out_ref[...] = total + sum_ref[0][...] if partner else total


def factor_kernel(n_dp, *refs):
    inverse_ref, gram_ref, high_ref, low_ref = refs[2 * n_dp :]
    width = refs[0].shape[1]
    rank = refs[0].shape[0]
    total = jnp.zeros((3 * rank, 3 * rank), f32)
    for index in range(2 * n_dp):
        terms = jnp.concatenate(split3(refs[index][...]), axis=0)
        total += lax.dot_general(terms, terms, (((1,), (1,)), ((), ())), preferred_element_type=f32)
    gram = jnp.zeros((rank, rank), f32)
    for a in range(3):
        for b in range(3):
            gram += total[a * rank : (a + 1) * rank, b * rank : (b + 1) * rank]
    row_id = lax.broadcasted_iota(jnp.int32, (rank, rank), 0)
    col_id = lax.broadcasted_iota(jnp.int32, (rank, rank), 1)
    unit = (row_id == col_id).astype(f32)
    ridge = 1e-06 * jnp.sum(gram * unit) / rank
    both = jnp.concatenate([gram + ridge * unit, unit], axis=1)
    below = lax.broadcasted_iota(jnp.int32, (rank, 1), 0)
    for j in range(rank - 1):
        factor = both[:, j : j + 1] / both[j : j + 1, j : j + 1]
        both = both - jnp.where(below > j, factor, 0.0) * both[j : j + 1, :]
    pivots = jnp.sum(both[:, :rank] * unit, axis=1, keepdims=True)
    inverse = both[:, rank:] / jnp.sqrt(pivots)
    inverse_ref[...] = inverse
    gram_ref[...] = unit - ridge * lax.dot_general(
        inverse, inverse, (((1,), (1,)), ((), ())), precision=HIGHEST, preferred_element_type=f32
    )
    inverse2 = jnp.concatenate(split2(inverse), axis=0)
    for index in range(2 * n_dp):
        rows = piece_rows(n_dp, width, index % n_dp, index >= n_dp)
        high, low = split2(refs[index][...])
        first = jnp.dot(inverse2, high, preferred_element_type=f32)
        second = jnp.dot(inverse2[:rank], low, preferred_element_type=f32)
        high, low = split2(first[:rank] + (first[rank:] + second))
        high_ref[:, pl.ds(rows, width)] = high
        low_ref[:, pl.ds(rows, width)] = low


def solve_kernel(n_dp, inverse_ref, *refs):
    out_ref = refs[n_dp + 2]
    total = refs[0][...]
    for k in range(1, n_dp):
        total += refs[k][...]
    out_ref[...] = jnp.dot(
        inverse_ref[...], total / n_dp, precision=HIGHEST, preferred_element_type=f32
    )


def stacked_left(high, low):
    return jnp.concatenate([high, high, low], axis=0)


def stacked_right(right):
    high, low = split2(right)
    return jnp.concatenate([high, low, high], axis=0)


def product(left3, right3):
    return lax.dot_general(left3, right3, (((0,), (0,)), ((), ())), preferred_element_type=f32)


def residual_kernel(chunks, high_ref, low_ref, right_ref, merged_ref, out_ref, error_ref, sems):
    rows = error_ref.shape[0] // chunks
    right3 = stacked_right(right_ref[...])
    copies = []
    for i in range(chunks):
        place = pl.ds(i * rows, rows)
        update = product(stacked_left(high_ref[:, place], low_ref[:, place]), right3)
        error_ref[place, :] = (merged_ref[place, :].astype(f32) - update).astype(bf16)
        copy = pltpu.make_async_copy(error_ref.at[place, :], out_ref.at[0, place, :], sems.at[i])
        copy.start()
        copies.append(copy)
    for copy in copies:
        copy.wait()


def own_left(own, high_ref, low_ref):
    if own % 128:
        return stacked_left(high_ref[...], low_ref[...])
    place = lax.axis_index("dp") * lax.axis_size("shard") + lax.axis_index("shard")
    place = lanes(place * own, own, own)
    return stacked_left(high_ref[:, place], low_ref[:, place])


def gram_of(right3s):
    rank = right3s[0].shape[0] // 3
    total = jnp.zeros((2 * rank, 2 * rank), f32)
    for right3 in right3s:
        terms = right3[: 2 * rank]
        total += lax.dot_general(terms, terms, (((1,), (1,)), ((), ())), preferred_element_type=f32)
    return total[:rank, :rank] + total[:rank, rank:] + total[rank:, :rank] + total[rank:, rank:]


def own_rows(update_ref, high_ref, low_ref, right3s):
    cols = right3s[0].shape[1]
    left = own_left(update_ref.shape[0], high_ref, low_ref)
    for k, right3 in enumerate(right3s):
        update_ref[:, k * cols : (k + 1) * cols] = product(left, right3)


def rows_kernel(high_ref, low_ref, *refs):
    *right_refs, update_ref, gram_ref = refs
    right3s = [stacked_right(ref[...]) for ref in right_refs]
    own_rows(update_ref, high_ref, low_ref, right3s)
    gram_ref[...] = gram_of(right3s)


def adam_kernel(n_z, clip_level, high_ref, low_ref, gram_ref, here_ref, here_gram_ref, *refs):
    right_refs = refs[:n_z]
    first_ref, second_ref, *outs = refs[n_z : n_z + 5]
    *bufs, there_ref, sems = refs[n_z + 5 :]
    cols = right_refs[0].shape[1]
    own = first_ref.shape[0]
    shard = lax.axis_index("shard")
    core, z = lax.rem(shard, CORES), shard // CORES
    right3s = [stacked_right(ref[...]) for ref in right_refs]
    square = (here_gram_ref[...] + gram_of(right3s)) * gram_ref[...]
    square = jnp.sum(jnp.sum(square, axis=0, keepdims=True), axis=1, keepdims=True)
    ratio = clip_level / jnp.maximum(jnp.sqrt(square), clip_level)
    first_factor = (1.0 - BETA_ONE) * ratio
    second_factor = (1.0 - BETA_TWO) * ratio * ratio
    step = min(ADAM_ROWS, own)

    def column_of(k, partner):
        owner = 1 - core if partner else core
        column = (from_peer(z, k, n_z) * CORES + owner) * cols
        return pl.ds(pl.multiple_of(column, cols), cols)

    def copies(rows, place, index):
        return [
            pltpu.make_async_copy(
                bufs[j].at[rows, place], outs[j].at[rows, place], sems.at[j, index]
            )
            for j in range(3)
        ]

    for partner, update_ref in ((0, here_ref), (1, there_ref)):
        if partner:
            own_rows(there_ref, high_ref, low_ref, right3s)

        def tile(t, carry):
            k, part = t // (own // step), lax.rem(t, own // step)
            rows = pl.ds(pl.multiple_of(part * step, step), step)
            place = column_of(k, partner)
            update = update_ref[rows, pl.ds(pl.multiple_of(k * cols, cols), cols)]
            first = BETA_ONE * first_ref[rows, place] + first_factor * update
            second = BETA_TWO * second_ref[rows, place] + second_factor * (update * update)
            bufs[0][rows, place] = first
            bufs[1][rows, place] = second
            bufs[2][rows, place] = first / (second * lax.rsqrt(second) + EPSILON)
            for copy in copies(rows, place, k + n_z * partner):
                copy.start()
            return carry

        lax.fori_loop(0, n_z * (own // step), tile, 0)
    for partner in range(CORES):
        for k in range(n_z):
            for copy in copies(pl.ds(0, own), column_of(k, partner), k + n_z * partner):
                copy.wait()


def local(gradient, error_buffer, right_init, first_moment, second_moment):
    n_dp = lax.axis_size("dp")
    n_shard = lax.axis_size("shard")
    n_z = n_shard // CORES
    depth, cols = gradient.shape[1:]
    rank = right_init.shape[1]
    half = depth // CORES
    width = half // n_dp
    own = first_moment.shape[0]
    total_cols = first_moment.shape[1]

    def swap_cores(x):
        return lax.ppermute(x, "shard", [(i, i ^ 1) for i in range(n_shard)])

    def send_dp(x, k):
        pairs = [(i, to_peer(i, k, n_dp)) for i in range(n_dp)]
        return lax.ppermute(x, "dp", pairs)

    def send_z(x, k):
        pairs = [(i, to_peer(i // CORES, k, n_z) * CORES + i % CORES) for i in range(n_shard)]
        return lax.ppermute(x, "shard", pairs)

    chunks = 8
    merged, mine, other = pl.pallas_call(
        functools.partial(merge_kernel, chunks),
        in_specs=[ANY] * 3,
        out_specs=[VMEM] * 3,
        out_shape=[
            pltpu.VMEM((depth, cols), bf16),
            pltpu.VMEM((rank, half), f32),
            pltpu.VMEM((rank, half), f32),
        ],
        scratch_shapes=[
            pltpu.VMEM((depth, cols), bf16),
            pltpu.VMEM((rank, cols), f32),
            pltpu.SemaphoreType.DMA((3, chunks)),
        ],
        compiler_params=params(12),
        cost_estimate=cost(4 * depth * cols * rank, 6 * depth * cols),
        name="merge",
    )(in_hbm(gradient), in_hbm(error_buffer), in_hbm(right_init.T))

    got = swap_cores(other)
    pieces = pl.pallas_call(
        functools.partial(cut_kernel, n_dp),
        in_specs=[VMEM, VMEM],
        out_specs=[VMEM] * n_dp,
        out_shape=[pltpu.VMEM((rank, width), f32)] * n_dp,
        compiler_params=params(4),
        name="cut",
    )(mine, got)
    partial = pieces[0]
    for arrived in [send_dp(pieces[k], k) for k in range(1, n_dp)]:
        partial = partial + arrived
    total = partial
    for arrived in [send_z(partial, k) for k in range(1, n_z)]:
        total = total + arrived
    total = total / n_dp
    here_lefts = [total] + [send_dp(total, k) for k in range(1, n_dp)]
    there_lefts = [swap_cores(x) for x in here_lefts]
    lefts = here_lefts + there_lefts

    right_part = ()
    for partner, pieces in enumerate((here_lefts, there_lefts)):
        right_part = pl.pallas_call(
            functools.partial(right_kernel, n_dp, partner),
            in_specs=[VMEM] * (n_dp + 1 + partner),
            out_specs=VMEM,
            out_shape=pltpu.VMEM((rank, cols), f32),
            compiler_params=params(8),
            cost_estimate=cost(3 * depth * cols * rank, depth * cols),
        )(*pieces, merged, *([right_part] if partner else []))
    right_parts = [right_part] + [send_dp(right_part, k) for k in range(1, n_dp)]
    inverse, gram, high, low = pl.pallas_call(
        functools.partial(factor_kernel, n_dp),
        in_specs=[VMEM] * (2 * n_dp),
        out_specs=[VMEM] * 4,
        out_shape=[
            pltpu.VMEM((rank, rank), f32),
            pltpu.VMEM((rank, rank), f32),
            pltpu.VMEM((rank, depth), bf16),
            pltpu.VMEM((rank, depth), bf16),
        ],
        compiler_params=params(8),
        cost_estimate=cost(200 * depth * rank * rank, depth * rank * 8),
        name="factor",
    )(*lefts)
    first_here, second_here = in_vmem(first_moment), in_vmem(second_moment)
    right = pl.pallas_call(
        functools.partial(solve_kernel, n_dp),
        in_specs=[VMEM] * (n_dp + 3),
        out_specs=VMEM,
        out_shape=pltpu.VMEM((rank, cols), f32),
        compiler_params=params(16),
        name="solve",
    )(inverse, *right_parts, first_here, second_here)

    swapped = [swap_cores(right)]
    rights = [right] + [send_z(right, k) for k in range(1, n_z)]
    residual_chunks = 8
    error_out = pl.pallas_call(
        functools.partial(residual_kernel, residual_chunks),
        in_specs=[VMEM] * 4,
        out_specs=ANY,
        out_shape=pltpu.HBM((1, depth, cols), bf16),
        scratch_shapes=[pltpu.VMEM((depth, cols), bf16), pltpu.SemaphoreType.DMA((residual_chunks,))],
        compiler_params=params(12),
        cost_estimate=cost(16 * depth * cols * rank, 4 * depth * cols),
        name="residual",
    )(high, low, right, in_vmem(merged))
    for k in range(1, n_z):
        rights[k], error_out = lax.optimization_barrier((rights[k], error_out))
        swapped.append(swap_cores(rights[k]))

    if own % 128:
        first_row = (lax.axis_index("dp") * n_shard + lax.axis_index("shard")) * own
        high = lax.dynamic_slice_in_dim(high, first_row, own, 1)
        low = lax.dynamic_slice_in_dim(low, first_row, own, 1)
    clip_level = CLIP_LEVEL * float(rank * (depth + total_cols)) ** 0.5
    here, here_gram = pl.pallas_call(
        rows_kernel,
        in_specs=[VMEM] * (2 + n_z),
        out_specs=[VMEM] * 2,
        out_shape=[pltpu.VMEM((own, n_z * cols), f32), pltpu.VMEM((rank, rank), f32)],
        compiler_params=params(8),
        cost_estimate=cost(16 * own * total_cols * rank, 4 * own * total_cols),
        name="rows",
    )(high, low, *rights)
    first_out, second_out, direction = pl.pallas_call(
        functools.partial(adam_kernel, n_z, clip_level),
        in_specs=[VMEM] * (7 + n_z),
        out_specs=[ANY] * 3,
        out_shape=[pltpu.HBM(first_moment.shape, f32)] * 3,
        scratch_shapes=[pltpu.VMEM(first_moment.shape, f32)] * 3
        + [
            pltpu.VMEM((own, n_z * cols), f32),
            pltpu.SemaphoreType.DMA((3, n_shard)),
        ],
        compiler_params=params(24),
        cost_estimate=cost(16 * own * total_cols * rank, 20 * own * total_cols),
        name="adam",
    )(high, low, gram, here, here_gram, *swapped, first_here, second_here)
    return (error_out, first_out, second_out, direction)


def solution(mesh):
    return jax.shard_map(
        local,
        mesh=mesh,
        in_specs=(
            P("dp", None, "shard"),
            P("dp", None, "shard"),
            P("shard", None),
            P(("dp", "shard"), None),
            P(("dp", "shard"), None),
        ),
        out_specs=(
            P("dp", None, "shard"),
            P(("dp", "shard"), None),
            P(("dp", "shard"), None),
            P(("dp", "shard"), None),
        ),
        check_vma=False,
    )
```
